512 devices in a mesh: row: 64 (over y, z_lo, x), col: 8 (over z_hi, core).
Axes of the slice: x: 4, y: 4, z: 16 (z_hi: 4, z_lo: 4; z = z_hi * 4 + z_lo), core: 2. Of those that a mesh axis runs over, the one named last changes fastest.
Arguments:
- environment: float32 [6144, 6144], P('row', 'col'), may hold values from -6 to 6
- site_tensors: float32 [2, 6144, 6144], P(None, 'row', 'col'), may hold values from -0.078125 to 0.078125
- panel_offset: int32 [1], replicated, may hold values from 0 to 6016
Outputs:
- new_panel: float32 [128, 6144], P('row', 'col')
The draws below stay inside these ranges and needn't reach their ends.
All inputs are finite; a program needn't handle non-finite values.
Results may differ from the reference program's by a relative error of at most 0.0001.
Values sent between devices are 32-bit elements; how exact they have to be, the bound alone decides.
No kernel may reach another device: no remote copies, remote signals or barrier semaphores. Data moves between devices by JAX's collectives and lax.ppermute only.
A program may use at most 64 MiB of HBM per device.

```python
import jax
import jax.numpy as jnp
from jax import lax

D = 6144
PHYS = 2
PANEL = 128


def block_levels(key, extent, cuts, least, high):
    def one(position, parts):
        heights = jax.random.uniform(jax.random.fold_in(jax.random.fold_in(key, 6), position), (parts,), jnp.float32, least / len(cuts), high / len(cuts))
        return jnp.repeat(jnp.exp(heights), extent[position] // parts).reshape((-1,) + (1,) * (len(extent) - position - 1))

    loudness = one(*cuts[0])
    for cut in cuts[1:]:
        loudness = loudness * one(*cut)
    return loudness


def bell_draw(own_key, shape, width, limit, shards=(), held_as=jnp.bfloat16):
    values = jax.random.normal(own_key, shape, jnp.float32) * width
    if len(shards) > 0:
        values = block_levels(own_key, shape, shards, -0.22, 0.18) * values
    return jnp.clip(values, min=-limit, max=limit).astype(held_as)


def setup_inputs(seed: int = 0) -> dict:
    seeds = jax.random.split(jax.random.key(seed), 4)
    return {
        "environment": bell_draw(seeds[0], (D, D), 1.0, 6.0, ((0, 64), (1, 8)), jnp.float32),
        "site_tensors": bell_draw(seeds[1], (PHYS, D, D), D ** -0.5, 0.078125, ((1, 64), (2, 8)), jnp.float32),
        "panel_offset": jax.random.randint(seeds[2], (1,), 0, D - PANEL + 1).astype(jnp.int32),
    }


def reference(environment, site_tensors, panel_offset):
    result = jnp.zeros((PANEL, D), jnp.float32)
    for phys in range(PHYS):
        columns = lax.dynamic_slice_in_dim(site_tensors[phys], panel_offset[0].astype(jnp.int32), PANEL, 1)
        bond_block = jnp.dot(columns.T, environment, precision=lax.Precision.HIGHEST, preferred_element_type=jnp.float32)
        result = result + jnp.dot(bond_block, site_tensors[phys], precision=lax.Precision.HIGHEST, preferred_element_type=jnp.float32)
    return result
```

```python
import jax
import jax.numpy as jnp
from jax import lax
from jax.sharding import Mesh, PartitionSpec as P

PHYS = 2
PANEL = 128
ROW = ("y", "zl", "x")
COL = ("zh", "core")
ALL = ROW + COL
SIZES = (4, 4, 4, 4, 2)
HOP = (3, 0, 2, 1)


def flat(y, zl, x, zh, core):
    return (((y * 4 + zl) * 4 + x) * 4 + zh) * 2 + core


def deliveries():
    pairs = []
    for y in range(4):
        s, b = y // 2, y % 2
        for zl in range(4):
            for x in range(4):
                for zh in range(4):
                    for core in range(2):
                        there = flat(zh, 2 * core + b, x, (zh + HOP[zl]) % 4, s)
                        pairs.append((flat(y, zl, x, zh, core), there))
    return pairs


def shards(environment, site_tensors, panel_offset):
    rows = environment.shape[0]
    cols = environment.shape[1]
    col_index = lax.axis_index(COL)
    core = lax.axis_index("core")
    padded = jnp.pad(site_tensors, ((0, 0), (0, 0), (PANEL, PANEL)))
    start = jnp.clip(panel_offset[0] - col_index * cols + PANEL, 0, cols + PANEL)
    window = lax.dynamic_slice_in_dim(padded, start, PANEL, 2)
    panel = lax.all_gather(window, COL).sum(axis=0)
    partial = jnp.einsum("ij,sip->sjp", environment, panel, precision=lax.Precision.HIGHEST)
    pieces = partial.reshape(16, rows, PANEL)
    pieces = lax.all_to_all(pieces, ("y", "x"), 0, 0, tiled=True)
    piece = pieces.sum(axis=0)
    piece = lax.all_gather(piece, "zl").sum(axis=0)
    mine = lax.ppermute(piece, ALL, deliveries())
    other = lax.ppermute(mine, "core", [(0, 1), (1, 0)])

    def times(block, phys):
        tensor = lax.dynamic_index_in_dim(site_tensors, phys, 0, keepdims=False)
        return jnp.einsum("jp,jm->pm", block, tensor, precision=lax.Precision.HIGHEST)

    total = times(mine, core) + times(other, 1 - core)
    shares = lax.all_to_all(total.reshape(64, 2, cols), ROW, 0, 0, tiled=True)
    return shares.sum(axis=0)


def solution(mesh):
    fine = Mesh(mesh.devices.reshape(SIZES), ALL)
    return jax.shard_map(
        shards,
        mesh=fine,
        in_specs=(P(ROW, COL), P(None, ROW, COL), P()),
        out_specs=P(ROW, COL),
        check_vma=False,
    )
```

```python
import jax
import jax.numpy as jnp
from jax import lax
from jax.sharding import Mesh, PartitionSpec as P

PHYS = 2
PANEL = 128
ROW = ("y", "zl", "x")
COL = ("zh", "core")
ALL = ROW + COL
SIZES = (4, 4, 4, 4, 2)
HOPS = ((3, 0, 1, 2), (3, 0, 1, 2), (2, 3, 0, 1), (2, 3, 0, 1))


def flat(y, zl, x, zh, core):
    return (((y * 4 + zl) * 4 + x) * 4 + zh) * 2 + core


def deliveries():
    pairs = []
    for y in range(4):
        s, b = y // 2, y % 2
        for zl in range(4):
            for x in range(4):
                for zh in range(4):
                    for core in range(2):
                        to = 2 * core + b
                        there = flat(zh, to, x, (zh + HOPS[to][zl]) % 4, s)
                        pairs.append((flat(y, zl, x, zh, core), there))
    return pairs


def shards(environment, site_tensors, panel_offset):
    rows = environment.shape[0]
    cols = environment.shape[1]
    col_index = lax.axis_index(COL)
    core = lax.axis_index("core")
    padded = jnp.pad(site_tensors, ((0, 0), (0, 0), (PANEL, PANEL)))
    start = jnp.clip(panel_offset[0] - col_index * cols + PANEL, 0, cols + PANEL)
    window = lax.dynamic_slice_in_dim(padded, start, PANEL, 2)
    panel = lax.all_gather(window, COL).sum(axis=0)
    partial = jnp.einsum("ij,sip->sjp", environment, panel, precision=lax.Precision.HIGHEST)
    pieces = partial.reshape(16, rows, PANEL)
    pieces = lax.all_to_all(pieces, ("y", "x"), 0, 0, tiled=True)
    piece = pieces.sum(axis=0)
    copies = jnp.broadcast_to(piece[None], (4, rows, PANEL))
    piece = lax.all_to_all(copies, "zl", 0, 0, tiled=True).sum(axis=0)
    mine = lax.ppermute(piece, ALL, deliveries())
    other = lax.ppermute(mine, "core", [(0, 1), (1, 0)])

    def times(block, phys):
        tensor = lax.dynamic_index_in_dim(site_tensors, phys, 0, keepdims=False)
        return jnp.einsum("jp,jm->pm", block, tensor, precision=lax.Precision.HIGHEST)

    total = times(mine, core) + times(other, 1 - core)
    shares = lax.all_to_all(total.reshape(64, 2, cols), ROW, 0, 0, tiled=True)
    return shares.sum(axis=0)


def solution(mesh):
    fine = Mesh(mesh.devices.reshape(SIZES), ALL)
    return jax.shard_map(
        shards,
        mesh=fine,
        in_specs=(P(ROW, COL), P(None, ROW, COL), P()),
        out_specs=P(ROW, COL),
        check_vma=False,
    )
```

```python
import jax
import jax.numpy as jnp
from jax import lax
from jax.sharding import Mesh, PartitionSpec as P

PHYS = 2
PANEL = 128
ROW = ("y", "zl", "x")
COL = ("zh", "core")
ALL = ROW + COL
SIZES = (4, 4, 4, 4, 2)
HOPS = ((3, 0, 1, 2), (3, 0, 1, 2), (2, 3, 0, 1), (2, 3, 0, 1))


def flat(y, zl, x, zh, core):
    return (((y * 4 + zl) * 4 + x) * 4 + zh) * 2 + core


def deliveries():
    pairs = []
    for y in range(4):
        far, b = y // 2, y % 2
        for zl in range(4):
            for x in range(4):
                for zh in range(4):
                    for core in range(2):
                        to = 2 * (core ^ far) + b
                        there = flat(zh, to, x, (zh + HOPS[to][zl]) % 4, core)
                        pairs.append((flat(y, zl, x, zh, core), there))
    return pairs


def swap(values):
    return lax.ppermute(values, "core", [(0, 1), (1, 0)])


def shards(environment, site_tensors, panel_offset):
    rows = environment.shape[0]
    cols = environment.shape[1]
    col_index = lax.axis_index(COL)
    core = lax.axis_index("core")
    padded = jnp.pad(site_tensors, ((0, 0), (0, 0), (PANEL, PANEL)))
    start = jnp.clip(panel_offset[0] - col_index * cols + PANEL, 0, cols + PANEL)
    zero = jnp.zeros_like(start)

    def window(phys):
        return lax.dynamic_slice(padded, (phys, zero, start), (1, rows, PANEL))[0]

    sent = jnp.concatenate([window(1 - core), environment], axis=1)
    came = swap(sent)
    half = window(core) + came[:, :PANEL]
    panel = lax.all_gather(half, "zh").sum(axis=0)

    def bond(block):
        return jnp.einsum("ij,ip->jp", block, panel, precision=lax.Precision.HIGHEST)

    pieces = jnp.concatenate([bond(environment), bond(came[:, PANEL:])], axis=0)
    pieces = pieces.reshape(16, rows, PANEL)
    pieces = lax.all_to_all(pieces, ("y", "x"), 0, 0, tiled=True)
    piece = pieces.sum(axis=0)
    copies = jnp.broadcast_to(piece[None], (4, rows, PANEL))
    piece = lax.all_to_all(copies, "zl", 0, 0, tiled=True).sum(axis=0)
    mine = lax.ppermute(piece, ALL, deliveries())
    other = swap(mine)

    def times(block, phys):
        tensor = lax.dynamic_index_in_dim(site_tensors, phys, 0, keepdims=False)
        return jnp.einsum("jp,jm->pm", block, tensor, precision=lax.Precision.HIGHEST)

    total = times(mine, core) + times(other, 1 - core)
    shares = lax.all_to_all(total.reshape(64, 2, cols), ROW, 0, 0, tiled=True)
    return shares.sum(axis=0)


def solution(mesh):
    fine = Mesh(mesh.devices.reshape(SIZES), ALL)
    return jax.shard_map(
        shards,
        mesh=fine,
        in_specs=(P(ROW, COL), P(None, ROW, COL), P()),
        out_specs=P(ROW, COL),
        check_vma=False,
    )
```

```python
import jax
import jax.numpy as jnp
from jax import lax
from jax.sharding import Mesh, PartitionSpec as P

PHYS = 2
PANEL = 128
ROW = ("y", "zl", "x")
COL = ("zh", "core")
ALL = ROW + COL
SIZES = (4, 4, 4, 4, 2)
HOPS = ((3, 0, 1, 2), (3, 0, 1, 2), (2, 3, 0, 1), (2, 3, 0, 1))


def flat(y, zl, x, zh, core):
    return (((y * 4 + zl) * 4 + x) * 4 + zh) * 2 + core


def deliveries():
    pairs = []
    for y in range(4):
        far, b = y // 2, y % 2
        for zl in range(4):
            for x in range(4):
                for zh in range(4):
                    for core in range(2):
                        to = 2 * (core ^ far) + b
                        there = flat(zh, to, x, (zh + HOPS[to][zl]) % 4, core)
                        pairs.append((flat(y, zl, x, zh, core), there))
    return pairs


def swap(values):
    return lax.ppermute(values, "core", [(0, 1), (1, 0)])


ROUTES = (((2, 1, 3), None), ((0, 2), (2, 3)), ((0, 1, 3), None), ((1, 0, 2), None))


def from_cube(owner):
    targets, relay = ROUTES[owner]

    def spread(half):
        held = jnp.where(lax.axis_index("zh") == owner, half, jnp.zeros_like(half))
        for part in [lax.ppermute(half, "zh", [(owner, to)]) for to in targets]:
            held = held + part
        if relay:
            held = held + lax.ppermute(held, "zh", [relay])
        return held

    return spread


def from_all_cubes(half):
    return lax.all_gather(half, "zh").sum(axis=0)


def panel_of(half, offset, cols):
    first = offset // (2 * cols)
    last = (offset + PANEL - 1) // (2 * cols)
    case = jnp.where(first == last, first, 4)
    return lax.switch(case, [from_cube(zh) for zh in range(4)] + [from_all_cubes], half)


def shards(environment, site_tensors, panel_offset):
    rows = environment.shape[0]
    cols = environment.shape[1]
    col_index = lax.axis_index(COL)
    core = lax.axis_index("core")
    padded = jnp.pad(site_tensors, ((0, 0), (0, 0), (PANEL, PANEL)))
    start = jnp.clip(panel_offset[0] - col_index * cols + PANEL, 0, cols + PANEL)
    zero = jnp.zeros_like(start)

    def window(phys):
        return lax.dynamic_slice(padded, (phys, zero, start), (1, rows, PANEL))[0]

    sent = jnp.concatenate([window(1 - core), environment], axis=1)
    came = swap(sent)
    half = window(core) + came[:, :PANEL]
    panel = panel_of(half, panel_offset[0], cols)

    def bond(block):
        return jnp.einsum("ij,ip->jp", block, panel, precision=lax.Precision.HIGHEST)

    pieces = jnp.concatenate([bond(environment), bond(came[:, PANEL:])], axis=0)
    pieces = pieces.reshape(16, rows, PANEL)
    pieces = lax.all_to_all(pieces, ("y", "x"), 0, 0, tiled=True)
    piece = pieces.sum(axis=0)
    copies = jnp.broadcast_to(piece[None], (4, rows, PANEL))
    piece = lax.all_to_all(copies, "zl", 0, 0, tiled=True).sum(axis=0)
    mine = lax.ppermute(piece, ALL, deliveries())
    other = swap(mine)

    def times(block, phys):
        tensor = lax.dynamic_index_in_dim(site_tensors, phys, 0, keepdims=False)
        return jnp.einsum("jp,jm->pm", block, tensor, precision=lax.Precision.HIGHEST)

    total = times(mine, core) + times(other, 1 - core)
    shares = lax.all_to_all(total.reshape(64, 2, cols), ROW, 0, 0, tiled=True)
    return shares.sum(axis=0)


def solution(mesh):
    fine = Mesh(mesh.devices.reshape(SIZES), ALL)
    return jax.shard_map(
        shards,
        mesh=fine,
        in_specs=(P(ROW, COL), P(None, ROW, COL), P()),
        out_specs=P(ROW, COL),
        check_vma=False,
    )
```

```python
import jax
import jax.numpy as jnp
from jax import lax
from jax.experimental import pallas as pl
from jax.experimental.pallas import tpu as pltpu
from jax.sharding import Mesh, PartitionSpec as P

PHYS = 2
PANEL = 128
ROW = ("y", "zl", "x")
COL = ("zh", "core")
ALL = ROW + COL
SIZES = (4, 4, 4, 4, 2)
HOPS = ((3, 0, 1, 2), (3, 0, 1, 2), (2, 3, 0, 1), (2, 3, 0, 1))


def flat(y, zl, x, zh, core):
    return (((y * 4 + zl) * 4 + x) * 4 + zh) * 2 + core


SHIFT = (2, 0, 3, 1)
TARGET = (1, 3, 0, 2)


def deliveries():
    pairs = []
    for y in range(4):
        for zl in range(4):
            for x in range(4):
                for zh in range(4):
                    to = TARGET[(y - zh) % 4]
                    for core in range(2):
                        there = flat(zh, to, x, (zh + HOPS[to][zl]) % 4, core)
                        pairs.append((flat(y, zl, x, zh, core), there))
    return pairs


SMALL = pltpu.CompilerParams(vmem_limit_bytes=8 * 2**20)


def halves(values):
    high = values.astype(jnp.bfloat16)
    return high, (values - high.astype(jnp.float32)).astype(jnp.bfloat16)


def product(left, right):
    dot = lambda a, b: jnp.dot(a, b, preferred_element_type=jnp.float32)
    (lh, ll), (rh, rl) = halves(left), halves(right)
    return dot(lh, rh) + (dot(lh, rl) + dot(ll, rh))


def bond_kernel(panel_ref, sent_ref, came_ref, out_ref):
    core, zh = lax.axis_index("core"), lax.axis_index("zh")
    panel = panel_ref[...].T
    count = out_ref.shape[1]
    for far, ref in ((0, sent_ref), (1, came_ref)):
        block = product(panel, ref[:, PANEL:])
        for b in range(2):
            to = 2 * (core ^ far) + b
            shift = jnp.where(to == 0, 2, jnp.where(to == 1, 0, jnp.where(to == 2, 3, 1)))
            y = (zh + shift) % 4
            for x in range(4):
                start = (4 * b + x) * count
                out_ref[4 * y + x] = block[:, start : start + count].T


def bond(panel, sent, came):
    rows = panel.shape[0]
    return pl.pallas_call(
        bond_kernel,
        out_shape=jax.ShapeDtypeStruct((16, rows, PANEL), jnp.float32),
        in_specs=[pl.BlockSpec(memory_space=pltpu.VMEM)] * 3,
        out_specs=pl.BlockSpec(memory_space=pltpu.VMEM),
        compiler_params=SMALL,
        name="bond",
    )(panel, sent, came)


def mine_kernel(block_ref, tensors_ref, out_ref):
    core = lax.axis_index("core")
    out_ref[...] = product(block_ref[...].T, tensors_ref[core])


def other_kernel(block_ref, tensors_ref, sum_ref, out_ref):
    core = lax.axis_index("core")
    total = sum_ref[...] + product(block_ref[...].T, tensors_ref[1 - core])
    out_ref[...] = total.reshape(out_ref.shape)


def times(kernel, shape, *operands):
    return pl.pallas_call(
        kernel,
        out_shape=jax.ShapeDtypeStruct(shape, jnp.float32),
        in_specs=[pl.BlockSpec(memory_space=pltpu.VMEM)] * len(operands),
        out_specs=pl.BlockSpec(memory_space=pltpu.VMEM),
        compiler_params=SMALL,
        name=kernel.__name__,
    )(*operands)


def add_kernel(shares_ref, out_ref):
    out_ref[...] = jnp.sum(shares_ref[...], axis=0)


def swap(values):
    return lax.ppermute(values, "core", [(0, 1), (1, 0)])


ROUTES = (((2, 1, 3), None), ((0, 2), (2, 3)), ((0, 1, 3), None), ((1, 0, 2), None))


def from_cube(owner):
    targets, relay = ROUTES[owner]

    def spread(half):
        held = jnp.where(lax.axis_index("zh") == owner, half, jnp.zeros_like(half))
        for part in [lax.ppermute(half, "zh", [(owner, to)]) for to in targets]:
            held = held + part
        if relay:
            held = held + lax.ppermute(held, "zh", [relay])
        return held

    return spread


def from_all_cubes(half):
    return lax.all_gather(half, "zh").sum(axis=0)


def panel_of(half, offset, cols):
    first = offset // (2 * cols)
    last = (offset + PANEL - 1) // (2 * cols)
    case = jnp.where(first == last, first, 4)
    return lax.switch(case, [from_cube(zh) for zh in range(4)] + [from_all_cubes], half)


def shards(environment, site_tensors, panel_offset):
    rows = environment.shape[0]
    cols = environment.shape[1]
    col_index = lax.axis_index(COL)
    core = lax.axis_index("core")
    padded = jnp.pad(site_tensors, ((0, 0), (0, 0), (PANEL, PANEL)))
    start = jnp.clip(panel_offset[0] - col_index * cols + PANEL, 0, cols + PANEL)
    zero = jnp.zeros_like(start)

    def window(phys):
        return lax.dynamic_slice(padded, (phys, zero, start), (1, rows, PANEL))[0]

    sent = jnp.concatenate([window(1 - core), environment], axis=1)
    came = swap(sent)
    half = window(core) + came[:, :PANEL]
    panel = panel_of(half, panel_offset[0], cols)

    pieces = bond(panel, sent, came)
    pieces = lax.all_to_all(pieces, ("y", "x"), 0, 0, tiled=True)
    piece = pieces.sum(axis=0)
    copies = jnp.broadcast_to(piece[None], (4, rows, PANEL))
    piece = lax.all_to_all(copies, "zl", 0, 0, tiled=True).sum(axis=0)
    mine = lax.ppermute(piece, ALL, deliveries())
    other = swap(mine)

    total = times(mine_kernel, (PANEL, cols), mine, site_tensors)
    total = times(other_kernel, (64, 2, cols), other, site_tensors, total)
    shares = lax.all_to_all(total, ROW, 0, 0, tiled=True)
    return times(add_kernel, (2, cols), shares)


def solution(mesh):
    fine = Mesh(mesh.devices.reshape(SIZES), ALL)
    return jax.shard_map(
        shards,
        mesh=fine,
        in_specs=(P(ROW, COL), P(None, ROW, COL), P()),
        out_specs=P(ROW, COL),
        check_vma=False,
    )
```

```python
import jax
import jax.numpy as jnp
from jax import lax
from jax.experimental import pallas as pl
from jax.experimental.pallas import tpu as pltpu
from jax.sharding import Mesh, PartitionSpec as P


PANEL = 128
ROW = ("y", "zl", "x")
COL = ("zh", "core")
ALL = ROW + COL
SIZES = (4, 4, 4, 4, 2)
HOPS = ((3, 0, 1, 2), (3, 0, 1, 2), (2, 3, 0, 1), (2, 3, 0, 1))


def flat(y, zl, x, zh, core):
    return (((y * 4 + zl) * 4 + x) * 4 + zh) * 2 + core


TARGET = (1, 3, 0, 2)


def deliveries():
    pairs = []
    for y in range(4):
        for zl in range(4):
            for x in range(4):
                for zh in range(4):
                    to = TARGET[(y - zh) % 4]
                    for core in range(2):
                        there = flat(zh, to, x, (zh + HOPS[to][zl]) % 4, core)
                        pairs.append((flat(y, zl, x, zh, core), there))
    return pairs


SMALL = pltpu.CompilerParams(vmem_limit_bytes=8 * 2**20)


def halves(values):
    high = values.astype(jnp.bfloat16)
    return high, (values - high.astype(jnp.float32)).astype(jnp.bfloat16)


def product(left, right):
    dot = lambda a, b: jnp.dot(a, b, preferred_element_type=jnp.float32)
    (lh, ll), (rh, rl) = halves(left), halves(right)
    return dot(lh, rh) + (dot(lh, rl) + dot(ll, rh))


def bond_kernel(panel_ref, own_ref, came_ref, out_ref):
    core, zh = lax.axis_index("core"), lax.axis_index("zh")
    panel = panel_ref[...].T
    count = out_ref.shape[1]
    for far, ref in ((0, own_ref), (1, came_ref)):
        block = product(panel, ref[...])
        for b in range(2):
            to = 2 * (core ^ far) + b
            shift = jnp.where(to == 0, 2, jnp.where(to == 1, 0, jnp.where(to == 2, 3, 1)))
            y = (zh + shift) % 4
            for x in range(4):
                start = (4 * b + x) * count
                out_ref[4 * y + x] = block[:, start : start + count].T


def bond(panel, own, came):
    rows = panel.shape[0]
    return pl.pallas_call(
        bond_kernel,
        out_shape=jax.ShapeDtypeStruct((16, rows, PANEL), jnp.float32),
        in_specs=[pl.BlockSpec(memory_space=pltpu.VMEM)] * 3,
        out_specs=pl.BlockSpec(memory_space=pltpu.VMEM),
        compiler_params=SMALL,
        name="bond",
    )(panel, own, came)


def mine_kernel(block_ref, tensors_ref, out_ref):
    core = lax.axis_index("core")
    out_ref[...] = product(block_ref[...].T, tensors_ref[core])


def other_kernel(block_ref, tensors_ref, sum_ref, out_ref):
    core = lax.axis_index("core")
    total = sum_ref[...] + product(block_ref[...].T, tensors_ref[1 - core])
    out_ref[...] = total.reshape(out_ref.shape)


def times(kernel, shape, *operands):
    return pl.pallas_call(
        kernel,
        out_shape=jax.ShapeDtypeStruct(shape, jnp.float32),
        in_specs=[pl.BlockSpec(memory_space=pltpu.VMEM)] * len(operands),
        out_specs=pl.BlockSpec(memory_space=pltpu.VMEM),
        compiler_params=SMALL,
    )(*operands)


def add_kernel(shares_ref, out_ref):
    out_ref[...] = jnp.sum(shares_ref[...], axis=0)


TARGETS = ((1, 3, 2), (0, 2, 3), (0, 1, 3), (0, 1, 2))


def swap(values):
    return lax.ppermute(values, "core", [(0, 1), (1, 0)])


def from_cube(owner):
    def spread(kept, sent, environment):
        pair = [(2 * owner, 2 * owner + 1), (2 * owner + 1, 2 * owner)]
        half = kept + lax.ppermute(sent, COL, pair)
        held = jnp.where(lax.axis_index("zh") == owner, half, jnp.zeros_like(half))
        parts = [lax.ppermute(half, "zh", [(owner, to)]) for to in TARGETS[owner]]
        came = lax.ppermute(environment, "core", [(0, 1), (1, 0)])
        for part in parts:
            held = held + part
        return held, came

    return spread


def from_all_cubes(kept, sent, environment):
    half = kept + swap(sent)
    return lax.all_gather(half, "zh").sum(axis=0), swap(environment)


def panel_of(kept, sent, environment, offset):
    cols = 2 * environment.shape[1]
    first = offset // cols
    last = (offset + PANEL - 1) // cols
    case = jnp.where(first == last, first, 4)
    branches = [from_cube(zh) for zh in range(4)] + [from_all_cubes]
    return lax.switch(case, branches, kept, sent, environment)


def shards(environment, site_tensors, panel_offset):
    rows = environment.shape[0]
    cols = environment.shape[1]
    col_index = lax.axis_index(COL)
    core = lax.axis_index("core")
    padded = jnp.pad(site_tensors, ((0, 0), (0, 0), (PANEL, PANEL)))
    start = jnp.clip(panel_offset[0] - col_index * cols + PANEL, 0, cols + PANEL)
    zero = jnp.zeros_like(start)

    def window(phys):
        return lax.dynamic_slice(padded, (phys, zero, start), (1, rows, PANEL))[0]

    panel, came = panel_of(window(core), window(1 - core), environment, panel_offset[0])
    pieces = bond(panel, environment, came)
    pieces = lax.all_to_all(pieces, ("y", "x"), 0, 0, tiled=True)
    piece = pieces.sum(axis=0)
    copies = jnp.broadcast_to(piece[None], (4, rows, PANEL))
    piece = lax.all_to_all(copies, "zl", 0, 0, tiled=True).sum(axis=0)
    mine = lax.ppermute(piece, ALL, deliveries())
    other = swap(mine)

    total = times(mine_kernel, (PANEL, cols), mine, site_tensors)
    total = times(other_kernel, (64, 2, cols), other, site_tensors, total)
    shares = lax.all_to_all(total, ROW, 0, 0, tiled=True)
    return times(add_kernel, (2, cols), shares)


def solution(mesh):
    fine = Mesh(mesh.devices.reshape(SIZES), ALL)
    return jax.shard_map(
        shards,
        mesh=fine,
        in_specs=(P(ROW, COL), P(None, ROW, COL), P()),
        out_specs=P(ROW, COL),
        check_vma=False,
    )
```

```python
import jax
import jax.numpy as jnp
from jax import lax
from jax.experimental import pallas as pl
from jax.experimental.pallas import tpu as pltpu
from jax.sharding import Mesh, PartitionSpec as P


PANEL = 128
ROW = ("y", "zl", "x")
COL = ("zh", "core")
ALL = ROW + COL
SIZES = (4, 4, 4, 4, 2)
HOPS = ((3, 0, 1, 2), (3, 0, 1, 2), (2, 3, 0, 1), (2, 3, 0, 1))


def flat(y, zl, x, zh, core):
    return (((y * 4 + zl) * 4 + x) * 4 + zh) * 2 + core


TARGET = (1, 3, 0, 2)


def deliveries():
    pairs = []
    for y in range(4):
        for zl in range(4):
            for x in range(4):
                for zh in range(4):
                    to = TARGET[(y - zh) % 4]
                    for core in range(2):
                        there = flat(zh, to, x, (zh + HOPS[to][zl]) % 4, core)
                        pairs.append((flat(y, zl, x, zh, core), there))
    return pairs


SMALL = pltpu.CompilerParams(vmem_limit_bytes=8 * 2**20)


def halves(values):
    high = values.astype(jnp.bfloat16)
    return high, (values - high.astype(jnp.float32)).astype(jnp.bfloat16)


def product(left, right):
    dot = lambda a, b: jnp.dot(a, b, preferred_element_type=jnp.float32)
    (lh, ll), (rh, rl) = halves(left), halves(right)
    return dot(lh, rh) + (dot(lh, rl) + dot(ll, rh))


def bond_kernel(panel_ref, own_ref, came_ref, out_ref):
    core, zh = lax.axis_index("core"), lax.axis_index("zh")
    panel = panel_ref[...].T
    count = out_ref.shape[1]
    for far, ref in ((0, own_ref), (1, came_ref)):
        block = product(panel, ref[...])
        for b in range(2):
            to = 2 * (core ^ far) + b
            shift = jnp.where(to == 0, 2, jnp.where(to == 1, 0, jnp.where(to == 2, 3, 1)))
            y = (zh + shift) % 4
            for x in range(4):
                start = (4 * b + x) * count
                out_ref[4 * y + x] = block[:, start : start + count].T


def bond(panel, own, came):
    rows = panel.shape[0]
    return pl.pallas_call(
        bond_kernel,
        out_shape=jax.ShapeDtypeStruct((16, rows, PANEL), jnp.float32),
        in_specs=[pl.BlockSpec(memory_space=pltpu.VMEM)] * 3,
        out_specs=pl.BlockSpec(memory_space=pltpu.VMEM),
        compiler_params=SMALL,
        name="bond",
    )(panel, own, came)


def mine_kernel(block_ref, tensors_ref, out_ref):
    core = lax.axis_index("core")
    out_ref[...] = product(block_ref[...].T, tensors_ref[core])


def other_kernel(block_ref, tensors_ref, sum_ref, out_ref):
    core = lax.axis_index("core")
    total = sum_ref[...] + product(block_ref[...].T, tensors_ref[1 - core])
    out_ref[...] = total.reshape(out_ref.shape)


def times(kernel, shape, *operands):
    return pl.pallas_call(
        kernel,
        out_shape=jax.ShapeDtypeStruct(shape, jnp.float32),
        in_specs=[pl.BlockSpec(memory_space=pltpu.VMEM)] * len(operands),
        out_specs=pl.BlockSpec(memory_space=pltpu.VMEM),
        compiler_params=SMALL,
    )(*operands)


def add_kernel(shares_ref, out_ref):
    out_ref[...] = jnp.sum(shares_ref[...], axis=0)


CASES = (
    ((0,), (((0, 1),), ((0, 3),), ((0, 2),))),
    ((1,), (((1, 0),), ((1, 2),), ((1, 3),))),
    ((2,), (((2, 0),), ((2, 1),), ((2, 3),))),
    ((3,), (((3, 0),), ((3, 1),), ((3, 2),))),
    ((0, 1), (((0, 1), (1, 0)), ((0, 3), (1, 2)), ((0, 2), (1, 3)))),
    ((1, 2), (((1, 0), (2, 3)), ((1, 2), (2, 1)), ((2, 0), (1, 3)))),
    ((2, 3), (((2, 0), (3, 1)), ((3, 0), (2, 1)), ((2, 3), (3, 2)))),
)


def swap(values):
    return lax.ppermute(values, "core", [(0, 1), (1, 0)])


def from_owners(case):
    owners, permutes = CASES[case]

    def spread(kept, sent, environment):
        inside = [(2 * zh + core, 2 * zh + 1 - core) for zh in owners for core in range(2)]
        half = kept + lax.ppermute(sent, COL, inside)
        cube = lax.axis_index("zh")
        owned = (cube >= owners[0]) & (cube <= owners[-1])
        held = jnp.where(owned, half, jnp.zeros_like(half))
        parts = [lax.ppermute(half, "zh", pairs) for pairs in permutes]
        came = lax.ppermute(environment, "core", [(0, 1), (1, 0)])
        for part in parts:
            held = held + part
        return held, came

    return spread


def panel_of(kept, sent, environment, offset):
    cols = 2 * environment.shape[1]
    first = offset // cols
    last = (offset + PANEL - 1) // cols
    case = jnp.where(first == last, first, 4 + first)
    return lax.switch(case, [from_owners(n) for n in range(len(CASES))], kept, sent, environment)


def shards(environment, site_tensors, panel_offset):
    rows = environment.shape[0]
    cols = environment.shape[1]
    col_index = lax.axis_index(COL)
    core = lax.axis_index("core")
    padded = jnp.pad(site_tensors, ((0, 0), (0, 0), (PANEL, PANEL)))
    start = jnp.clip(panel_offset[0] - col_index * cols + PANEL, 0, cols + PANEL)
    zero = jnp.zeros_like(start)

    def window(phys):
        return lax.dynamic_slice(padded, (phys, zero, start), (1, rows, PANEL))[0]

    panel, came = panel_of(window(core), window(1 - core), environment, panel_offset[0])
    pieces = bond(panel, environment, came)
    pieces = lax.all_to_all(pieces, ("y", "x"), 0, 0, tiled=True)
    piece = pieces.sum(axis=0)
    copies = jnp.broadcast_to(piece[None], (4, rows, PANEL))
    piece = lax.all_to_all(copies, "zl", 0, 0, tiled=True).sum(axis=0)
    mine = lax.ppermute(piece, ALL, deliveries())
    other = swap(mine)

    total = times(mine_kernel, (PANEL, cols), mine, site_tensors)
    total = times(other_kernel, (64, 2, cols), other, site_tensors, total)
    shares = lax.all_to_all(total, ROW, 0, 0, tiled=True)
    return times(add_kernel, (2, cols), shares)


def solution(mesh):
    fine = Mesh(mesh.devices.reshape(SIZES), ALL)
    return jax.shard_map(
        shards,
        mesh=fine,
        in_specs=(P(ROW, COL), P(None, ROW, COL), P()),
        out_specs=P(ROW, COL),
        check_vma=False,
    )
```

```python
import jax
import jax.numpy as jnp
from jax import lax
from jax.experimental import pallas as pl
from jax.experimental.pallas import tpu as pltpu
from jax.sharding import Mesh, PartitionSpec as P


PANEL = 128
ROW = ("y", "zl", "x")
COL = ("zh", "core")
ALL = ROW + COL
SIZES = (4, 4, 4, 4, 2)
HOPS = ((3, 0, 1, 2), (3, 0, 1, 2), (2, 3, 0, 1), (2, 3, 0, 1))


def flat(y, zl, x, zh, core):
    return (((y * 4 + zl) * 4 + x) * 4 + zh) * 2 + core


TARGET = (1, 3, 0, 2)


def deliveries():
    pairs = []
    for y in range(4):
        for zl in range(4):
            for x in range(4):
                for zh in range(4):
                    to = TARGET[(y - zh) % 4]
                    for core in range(2):
                        there = flat(zh, to, x, (zh + HOPS[to][zl]) % 4, core)
                        pairs.append((flat(y, zl, x, zh, core), there))
    return pairs


SMALL = pltpu.CompilerParams(vmem_limit_bytes=8 * 2**20)


def halves(values):
    high = values.astype(jnp.bfloat16)
    return high, (values - high.astype(jnp.float32)).astype(jnp.bfloat16)


def product(left, right):
    return of_parts(*halves(left), *halves(right))


def of_parts(lh, ll, rh, rl):
    dot = lambda a, b: jnp.dot(a, b, preferred_element_type=jnp.float32)
    return dot(lh, rh) + (dot(lh, rl) + dot(ll, rh))


def bond_kernel(panel_ref, own_high, own_low, high_ref, low_ref, out_ref):
    core, zh = lax.axis_index("core"), lax.axis_index("zh")
    panel = halves(panel_ref[...].T)
    count = out_ref.shape[1]
    blocks = (own_high[...], own_low[...]), (high_ref[...], low_ref[...])
    for far in range(2):
        block = of_parts(*panel, *blocks[far])
        for b in range(2):
            to = 2 * (core ^ far) + b
            shift = jnp.where(to == 0, 2, jnp.where(to == 1, 0, jnp.where(to == 2, 3, 1)))
            y = (zh + shift) % 4
            for x in range(4):
                start = (4 * b + x) * count
                out_ref[4 * y + x] = block[:, start : start + count].T


def bond(panel, *parts):
    rows = panel.shape[0]
    return pl.pallas_call(
        bond_kernel,
        out_shape=jax.ShapeDtypeStruct((16, rows, PANEL), jnp.float32),
        in_specs=[pl.BlockSpec(memory_space=pltpu.VMEM)] * 5,
        out_specs=pl.BlockSpec(memory_space=pltpu.VMEM),
        compiler_params=SMALL,
        name="bond",
    )(panel, *parts)


def mine_kernel(block_ref, tensors_ref, out_ref):
    core = lax.axis_index("core")
    out_ref[...] = product(block_ref[...].T, tensors_ref[core])


def other_kernel(block_ref, tensors_ref, sum_ref, out_ref):
    core = lax.axis_index("core")
    total = sum_ref[...] + product(block_ref[...].T, tensors_ref[1 - core])
    out_ref[...] = total.reshape(out_ref.shape)


def times(kernel, shape, *operands):
    return pl.pallas_call(
        kernel,
        out_shape=jax.ShapeDtypeStruct(shape, jnp.float32),
        in_specs=[pl.BlockSpec(memory_space=pltpu.VMEM)] * len(operands),
        out_specs=pl.BlockSpec(memory_space=pltpu.VMEM),
        compiler_params=SMALL,
    )(*operands)


def add_kernel(shares_ref, out_ref):
    out_ref[...] = jnp.sum(shares_ref[...], axis=0)


CASES = (
    ((0,), (((0, 1),), ((0, 3),), ((0, 2),))),
    ((1,), (((1, 0),), ((1, 2),), ((1, 3),))),
    ((2,), (((2, 0),), ((2, 1),), ((2, 3),))),
    ((3,), (((3, 0),), ((3, 1),), ((3, 2),))),
    ((0, 1), (((0, 1), (1, 0)), ((0, 3), (1, 2)), ((0, 2), (1, 3)))),
    ((1, 2), (((1, 0), (2, 3)), ((1, 2), (2, 1)), ((2, 0), (1, 3)))),
    ((2, 3), (((2, 0), (3, 1)), ((3, 0), (2, 1)), ((2, 3), (3, 2)))),
)


def swap(values):
    return lax.ppermute(values, "core", [(0, 1), (1, 0)])


def rounded(values):
    high = lax.reduce_precision(values, 8, 7)
    return high.astype(jnp.bfloat16), (values - high).astype(jnp.bfloat16)


def from_owners(case):
    owners, permutes = CASES[case]

    def spread(kept, sent, environment):
        inside = [(2 * zh + core, 2 * zh + 1 - core) for zh in owners for core in range(2)]
        half = kept + lax.ppermute(sent, COL, inside)
        cube = lax.axis_index("zh")
        owned = (cube >= owners[0]) & (cube <= owners[-1])
        held = jnp.where(owned, half, jnp.zeros_like(half))
        parts = [lax.ppermute(half, "zh", pairs) for pairs in permutes]
        came = lax.ppermute(environment, "core", [(0, 1), (1, 0)])
        for part in parts:
            held = held + part
        return held, *rounded(environment), *rounded(came)

    return spread


def panel_of(kept, sent, environment, offset):
    cols = 2 * environment.shape[1]
    first = offset // cols
    last = (offset + PANEL - 1) // cols
    case = jnp.where(first == last, first, 4 + first)
    return lax.switch(case, [from_owners(n) for n in range(len(CASES))], kept, sent, environment)


def shards(environment, site_tensors, panel_offset):
    rows = environment.shape[0]
    cols = environment.shape[1]
    col_index = lax.axis_index(COL)
    core = lax.axis_index("core")
    padded = jnp.pad(site_tensors, ((0, 0), (0, 0), (PANEL, PANEL)))
    start = jnp.clip(panel_offset[0] - col_index * cols + PANEL, 0, cols + PANEL)
    zero = jnp.zeros_like(start)

    def window(phys):
        return lax.dynamic_slice(padded, (phys, zero, start), (1, rows, PANEL))[0]

    kept, sent = lax.optimization_barrier((window(core), window(1 - core)))
    panel, *parts = panel_of(kept, sent, environment, panel_offset[0])
    pieces = bond(panel, *parts)
    pieces = lax.all_to_all(pieces, ("y", "x"), 0, 0, tiled=True)
    piece = pieces.sum(axis=0)
    copies = jnp.broadcast_to(piece[None], (4, rows, PANEL))
    piece = lax.all_to_all(copies, "zl", 0, 0, tiled=True).sum(axis=0)
    mine = lax.ppermute(piece, ALL, deliveries())
    other = swap(mine)

    total = times(mine_kernel, (PANEL, cols), mine, site_tensors)
    total = times(other_kernel, (64, 2, cols), other, site_tensors, total)
    shares = lax.all_to_all(total, ROW, 0, 0, tiled=True)
    return times(add_kernel, (2, cols), shares)


def solution(mesh):
    fine = Mesh(mesh.devices.reshape(SIZES), ALL)
    return jax.shard_map(
        shards,
        mesh=fine,
        in_specs=(P(ROW, COL), P(None, ROW, COL), P()),
        out_specs=P(ROW, COL),
        check_vma=False,
    )
```
